256 devices in a mesh: section: 8 (over z), expert: 32 (over y, x, core).
Axes of the slice: x: 4, y: 4, z: 8, core: 2. Of those that a mesh axis runs over, the one named last changes fastest.
Arguments:
- hidden_in: bfloat16 [2, 256, 3584], P(None, 'expert'), may hold values from -6 to 6
- layer_gain: float32 [8, 3584], P('section'), may hold values from 0.25 to 1.75
- router: bfloat16 [8, 3584, 8], P('section'), may hold values from -0.09375 to 0.09375
- w_gate: bfloat16 [8, 3584, 16384], P('section', None, 'expert'), may hold values from -0.09375 to 0.09375
- w_up: bfloat16 [8, 3584, 16384], P('section', None, 'expert'), may hold values from -0.09375 to 0.09375
- w_down: bfloat16 [8, 16384, 3584], P('section', 'expert'), may hold values from -0.125 to 0.125
- final_gain: float32 [3584], replicated, may hold values from 0.25 to 1.75
- head: bfloat16 [65536, 3584], P(('section', 'expert')), may hold values from -18.775102 to 18.775102
- routing: int32 [8, 2, 256, 2], P('section', None, 'expert'), may hold values from 0 to 7, all different within a row; in each aligned block of 8 rows (0 to 7, 8 to 15, ..., all dimensions but the last counted through in order) at most 2 rows name the same one
- targets: int32 [2, 256], replicated, may hold values from 0 to 65535
- seq_ids: int32 [2, 256], replicated, may hold values from 0 to 3, never falling along the last dimension, each value on 1 to 128 neighbouring positions
Outputs:
- token_logprob: float32 [2, 256], P(None, 'expert')
- seq_mean: float32 [2, 4], replicated
The draws below stay inside these ranges and needn't reach their ends.
Inputs may be any that keep to these rules, and one draw needn't show every extreme that they name: `routing`: in each aligned block of 8 tokens (the tokens of one device) a token's 2 experts differ and no expert is named by more than 2 tokens; some expert is named by exactly 2. `seq_ids`: ids never fall along a micro-batch's tokens; each of the 4 ids occurs on 1 to 128 tokens, one on exactly 128.
All inputs are finite; a program needn't handle non-finite values.
Results may differ from the reference program's by a relative error of at most 0.014.
Values may be sent and summed in bfloat16 or wider, within the bound.
A program may use at most 64 MiB of HBM per device.

```python
import math
import jax
import jax.numpy as jnp
import numpy as np
from jax import lax

D = 3584
FF = 2048
FF_SPLIT = 4
TOP = 2
TOK_DEV = 8
MICRO = 2
SEQS = 4
LAYERS = 8
EXPERTS = 8
FF_DEV = 512
TOKENS = 256
VOCAB = 65536
CAP = 2
SEQ_MOST = 128
N_EXPERT = 32


def draw_head(key, part):
    keys = jax.random.split(jax.random.fold_in(key, 17), 2)
    base = jnp.clip(jax.random.normal(keys[0], (VOCAB, D), jnp.float32), -4.0, 4.0)
    position = jnp.arange(VOCAB, dtype=jnp.float32)[:, None] / VOCAB
    rising = 0.6 + 1.2 * position
    jitter = jax.random.uniform(keys[1], (VOCAB, 1), jnp.float32, 0.7, 1.3)
    values = base * (3.0 / math.sqrt(D)) * rising * jitter
    return values.astype(jnp.bfloat16)


def plant(array, rng, low, top_value):
    longest = array.shape.index(max(array.shape))
    spots = []
    for shift in (0, 1):
        where = [jax.random.randint(jax.random.fold_in(rng, axis), (), 0, length) for axis, length in enumerate(array.shape)]
        where[longest] = (where[longest] + shift) % array.shape[longest]
        spots.append(tuple(where))
    return array.at[spots[0]].set(low).at[spots[1]].set(top_value)


def block_scale(own_key, dims, cuts, low, high):
    level = 1.0
    for dim, blocks in cuts:
        steps = jax.random.uniform(jax.random.fold_in(jax.random.fold_in(own_key, 6), dim), (blocks,), jnp.float32, low / len(cuts), high / len(cuts))
        level = level * jnp.repeat(jnp.exp(steps), dims[dim] // blocks).reshape((-1,) + (1,) * (len(dims) - 1 - dim))
    return level


def cumulative_ranks(number_of, lean):
    loads = [(1 << 20) // math.isqrt(rank ** lean) + 1 for rank in range(1, number_of + 1)]
    deviation = 1 + sum(loads) // (1 << 30)
    return np.cumsum(np.array([max(1, weight // deviation) for weight in loads]))


def ranked(own_key, shape, number_of, slope):
    grid = cumulative_ranks(number_of, slope)
    pick = jax.random.randint(jax.random.fold_in(own_key, 1), shape, 0, int(grid[number_of - 1]))
    grade = jnp.searchsorted(jnp.asarray(grid, jnp.int32), pick, side="right")
    return jax.random.permutation(jax.random.fold_in(own_key, 2), number_of)[grade].astype(jnp.int32)


def split_up(amount, total, most, lean):
    loads = [(1 << 20) // math.isqrt(grade ** lean) + 1 for grade in range(2, amount + 1)]
    surplus, holding = total - most - (amount - 1), [1] * (amount - 1)
    while surplus > 0:
        movable = [i for i in range(amount - 1) if holding[i] < most]
        whole, left = sum([loads[i] for i in movable]), surplus
        for i in movable:
            extra = min(most - holding[i], max(1, left * loads[i] // whole), surplus)
            holding[i] = holding[i] + extra
            surplus = surplus - extra
    return np.array([most] + holding)


def ragged(rng, number_of, total, reach, skew):
    if number_of == 2:
        one = jax.random.randint(rng, (), max(1, total - reach), min(reach, total - 1) + 1)
        return jnp.stack([one, total - one])
    lengths = jnp.asarray(split_up(number_of, total, reach, skew), jnp.int32)
    twos = (number_of - 1) // 2
    giver, taker = lengths[1:1 + 2 * twos:2], lengths[2:2 + 2 * twos:2]
    slack = jnp.minimum(giver - 1, reach - taker)
    shifted = jax.random.randint(jax.random.fold_in(rng, 1), (twos,), 0, 1 << 20) % (slack + 1)
    lengths = lengths.at[1:1 + 2 * twos:2].set(giver - shifted).at[2:2 + 2 * twos:2].set(taker + shifted)
    return lengths[jax.random.permutation(jax.random.fold_in(rng, 2), number_of)]


def routed_block(key, own, number, rows, number_of, top, most, slope):
    order = jax.random.permutation(key, number_of)
    heavy_load, common = portions_of(number_of, rows * top, most, slope, True), portions_of(number_of, rows * top, most, slope, False)
    places = jnp.arange(number_of)

    def named(lengths, rotation):
        used = int((lengths > 0).sum())
        fixed = max(1, used // 4)
        shifted = fixed + (places - fixed + rotation * (used - fixed)) % max(1, number_of - fixed)
        return jnp.zeros((number_of,), jnp.int32).at[order[jnp.where(places < fixed, places, shifted)]].set(jnp.asarray(lengths, jnp.int32))

    lengths = jnp.where(number % 4 == 0, named(heavy_load, number // 4), named(common, number - number // 4 - 1))
    mixed = jax.random.permutation(jax.random.fold_in(own, 3), number_of)
    source_of, receiver = mixed[0:number_of // 2 * 2:2], mixed[1:number_of // 2 * 2:2]
    slack = jnp.minimum(lengths[source_of] - 1, most - lengths[receiver]) // 2
    slack = jnp.where((source_of == order[0]) | (receiver == order[0]) | (lengths[receiver] == 0), 0, jnp.maximum(slack, 0))
    shifted = jax.random.randint(jax.random.fold_in(own, 4), (number_of // 2,), 0, 1 << 20) % (slack + 1)
    lengths = lengths.at[source_of].add(-shifted).at[receiver].add(shifted)
    labels = jnp.searchsorted(jnp.cumsum(lengths), jnp.arange(rows * top), side="right").astype(jnp.int32)
    grid = labels.reshape(top, rows).T
    grid = grid[jax.random.permutation(jax.random.fold_in(own, 1), rows)]
    rotation = jax.random.randint(jax.random.fold_in(own, 2), (rows, 1), 0, top)
    return jnp.take_along_axis(grid, (jnp.arange(top)[None, :] + rotation) % top, axis=1)


def portions_of(count, total, most, slope, full):
    loads = [(1 << 20) // math.isqrt(standing ** slope) + 1 for standing in range(1, count + 1)]
    largest = most if full else min(most, max(-(-total // count), total * loads[0] // sum(loads)))
    least = 1 if total - largest >= count - 1 else 0
    given, rest = [largest] + [least] * (count - 1), total - largest - least * (count - 1)
    while rest > 0:
        candidates = [i for i in range(1, count) if given[i] < largest] or [i for i in range(1, count) if given[i] < most]
        mass, left = sum([loads[i] for i in candidates]), rest
        for i in candidates:
            extra = min(most - given[i], max(1, left * loads[i] // mass), rest)
            given[i] = given[i] + extra
            rest = rest - extra
    return np.array(given)


def noise(key, extent, width, bound, cuts=(), held_as=jnp.bfloat16):
    level = block_scale(key, extent, cuts, -0.22, 0.18) if cuts else 1.0
    result = jax.random.normal(key, extent, jnp.float32) * width * level
    return jnp.minimum(jnp.maximum(result, -bound), bound).astype(held_as)


def setup_inputs(seed: int = 0) -> dict:
    streams_of = jax.random.split(jax.random.key(seed), 12)
    hidden_in = noise(streams_of[0], (MICRO, TOKENS, D), 1.0, 6.0, ((1, 32),))
    layer_gain = jnp.clip(1.0 + 0.15 * jax.random.normal(streams_of[1], (LAYERS, D), jnp.float32), 0.25, 1.75)
    router = noise(streams_of[2], (LAYERS, D, EXPERTS), D ** -0.5, 0.09375, ((0, 8),))
    w_gate = noise(streams_of[3], (LAYERS, D, EXPERTS * FF), D ** -0.5, 0.09375, ((0, 8), (2, 32)))
    w_up = noise(streams_of[4], (LAYERS, D, EXPERTS * FF), D ** -0.5, 0.09375, ((0, 8), (2, 32)))
    w_down = noise(streams_of[5], (LAYERS, EXPERTS * FF, D), FF ** -0.5, 0.125, ((0, 8), (1, 32)))
    final_gain = jnp.clip(1.0 + 0.15 * jax.random.normal(streams_of[6], (D,), jnp.float32), 0.25, 1.75)
    head = draw_head(jax.random.fold_in(streams_of[11], 71), 0)
    routing_keys = jax.random.split(jax.random.fold_in(streams_of[8], 1), LAYERS * MICRO * TOKENS // TOK_DEV)
    routing_turns = jax.random.permutation(jax.random.fold_in(streams_of[8], 3), LAYERS * MICRO * TOKENS // TOK_DEV)
    routing = jax.vmap(lambda own, number: routed_block(jax.random.fold_in(streams_of[8], 2), own, number, TOK_DEV, EXPERTS, TOP, CAP, 2))(routing_keys, routing_turns).reshape((LAYERS, MICRO, TOKENS, TOP))
    targets = plant(ranked(streams_of[9], (MICRO, TOKENS), VOCAB, 2), jax.random.fold_in(streams_of[9], 3), 0, VOCAB - 1).astype(jnp.int32)
    seq_ids = jax.vmap(lambda own: jnp.searchsorted(jnp.cumsum(ragged(own, SEQS, TOKENS, SEQ_MOST, 1)), jnp.arange(TOKENS), side="right"))(jax.random.split(streams_of[10], MICRO)).reshape((MICRO, TOKENS)).astype(jnp.int32)
    return dict(hidden_in=hidden_in, layer_gain=layer_gain, router=router, w_gate=w_gate, w_up=w_up, w_down=w_down, final_gain=final_gain, head=head, routing=routing, targets=targets, seq_ids=seq_ids)


def rms_scale(states, gain):
    values = states.astype(jnp.float32)
    factor = lax.rsqrt(lax.optimization_barrier(jnp.mean(values * values, -1, keepdims=True)) + 1e-06)
    return values * factor * gain.astype(jnp.float32)

def run_expert(operands):
    packed_rows, gate_cols, up_cols, down_rows = operands
    gate_val = jnp.dot(packed_rows, gate_cols, preferred_element_type=jnp.float32)
    up_val = jnp.dot(packed_rows, up_cols, preferred_element_type=jnp.float32)
    inner = (jax.nn.silu(gate_val) * up_val).astype(jnp.bfloat16)
    count = inner.shape[0]
    pieces = jnp.einsum('rfk,fkd->rfd', inner.reshape(count, FF_SPLIT, FF_DEV).astype(jnp.float32), down_rows.reshape(FF_SPLIT, FF_DEV, D).astype(jnp.float32), precision=lax.Precision.HIGHEST)
    rounded = lax.optimization_barrier(pieces.astype(jnp.bfloat16))
    return lax.optimization_barrier(jnp.sum(rounded.astype(jnp.float32), 1))

def pick_rows(block_out, slot_index):
    return block_out[slot_index]

def expert_layer(states, gain, router, gate_w, up_w, down_w, route_ids):
    blocks = N_EXPERT
    normed = rms_scale(states, gain).astype(jnp.bfloat16)
    logits = jnp.dot(normed, router, preferred_element_type=jnp.float32)
    chosen = route_ids[:, :, None] == jnp.arange(EXPERTS, dtype=jnp.int32)[None, None, :]
    affinity = jax.nn.sigmoid(lax.optimization_barrier(jnp.sum(jnp.where(chosen, logits[:, None, :], 0.0), -1)))
    weight = affinity / lax.optimization_barrier(jnp.sum(affinity, -1, keepdims=True))
    flags = chosen.reshape(blocks, TOK_DEV * TOP, EXPERTS).astype(jnp.int32)
    ranks = jnp.cumsum(flags, 1) - flags
    slot_ids = lax.optimization_barrier(jnp.sum(ranks * flags, -1)).reshape(blocks, TOK_DEV, TOP)
    target_slot = (route_ids.reshape(blocks, TOK_DEV, TOP) * CAP + slot_ids).astype(jnp.int32)
    places = jnp.arange(EXPERTS * CAP, dtype=jnp.int32)
    table = jnp.any(places[None, :, None, None] == target_slot[:, None], -1).astype(jnp.float32)
    packed = jnp.einsum('bst,btd->bsd', table, normed.reshape(blocks, TOK_DEV, D).astype(jnp.float32), precision=lax.Precision.HIGHEST).astype(jnp.bfloat16)
    per_expert = packed.reshape(blocks, EXPERTS, CAP, D).transpose(1, 0, 2, 3).reshape(EXPERTS, blocks * CAP, D)
    gate_e = gate_w.reshape(D, EXPERTS, FF).transpose(1, 0, 2)
    up_e = up_w.reshape(D, EXPERTS, FF).transpose(1, 0, 2)
    down_e = down_w.reshape(EXPERTS, FF, D)
    outputs = lax.map(run_expert, (per_expert, gate_e, up_e, down_e))
    by_block = outputs.reshape(EXPERTS, blocks, CAP, D).transpose(1, 0, 2, 3).reshape(blocks, EXPERTS * CAP, D)
    picked = jax.vmap(pick_rows)(by_block, target_slot)
    mixed = lax.optimization_barrier(jnp.sum(weight.reshape(blocks, TOK_DEV, TOP)[..., None] * picked, 2)).reshape(TOKENS, D)
    return (states.astype(jnp.float32) + 2.5 * mixed).astype(jnp.bfloat16)

def reference(hidden_in, layer_gain, router, w_gate, w_up, w_down, final_gain, head, routing, targets, seq_ids):
    states = [hidden_in[micro_id] for micro_id in range(MICRO)]
    for level in range(LAYERS):
        states = [expert_layer(states[micro_id], layer_gain[level], router[level], w_gate[level], w_up[level], w_down[level], routing[level, micro_id]) for micro_id in range(MICRO)]
    stacked = jnp.stack(states)
    normed = rms_scale(stacked, final_gain).astype(jnp.bfloat16).reshape(MICRO * TOKENS, D)
    logits = jnp.dot(normed, head.T, preferred_element_type=jnp.float32).reshape(MICRO, TOKENS, VOCAB)
    peak = lax.optimization_barrier(jnp.max(logits, -1))
    total = lax.optimization_barrier(jnp.sum(jnp.exp(logits - peak[..., None]), -1))
    target_logit = jnp.take_along_axis(logits, targets[..., None].astype(jnp.int32), -1)[..., 0]
    logprob = target_logit - (peak + jnp.log(total))
    member = seq_ids[:, :, None] == jnp.arange(SEQS, dtype=jnp.int32)[None, None, :]
    sums = lax.optimization_barrier(jnp.sum(jnp.where(member, logprob[..., None], 0.0), 1))
    counts = lax.optimization_barrier(jnp.sum(member.astype(jnp.float32), 1))
    return (logprob, sums / counts)
```

```python
import jax
import jax.numpy as jnp
from jax import lax
from jax.experimental import pallas as pl
from jax.experimental.pallas import tpu as pltpu
from jax.sharding import PartitionSpec as P

SEQS = 4
CHIPS = 16
F32, BF16, I32 = jnp.float32, jnp.bfloat16, jnp.int32
MESH = pl.DeviceIdType.MESH


def iota(shape, axis):
    return lax.broadcasted_iota(I32, shape, axis)


def rms_scale(states, gain):
    values = states.astype(F32)
    factor = lax.rsqrt(jnp.mean(values * values, -1, keepdims=True) + 1e-06)
    return values * factor * gain


def layers_kernel(
    hidden, gain, router, routes, last_gain, wanted, own_ids, all_ids, gate_hbm, up_hbm, down_hbm, head_hbm,
    token_out, mean_out,
    gate, up, down, head, head_other, gathered, stat_out, stat_in, plane_out, plane_in, seq_out, seq_in, states, packed, mine, other, rows, inner, part, away, back, summed, ret, leaving,
    weight_sem, disp_send, disp_recv, pair_send, pair_recv, half_send, half_recv, ret_send, ret_recv,
    hop_send, hop_recv, head_send, head_recv, cast_send, cast_recv, all_send, all_recv, stat_send, stat_recv,
    plane_send, plane_recv, seq_send, seq_recv,
):
    micro_count, tok_count, width = hidden.shape
    section, member = lax.axis_index("section"), lax.axis_index("expert")
    sections, members = lax.axis_size("section"), lax.axis_size("expert")
    last = sections - 1
    chip, core = member // 2, member % 2
    partner = member + 1 - 2 * core

    loads = [
        pltpu.make_async_copy(source, target, weight_sem.at[k])
        for k, (source, target) in enumerate(((gate_hbm, gate), (up_hbm, up), (down_hbm, down), (head_hbm, head)))
    ]
    for load in loads:
        load.start()

    barrier = pltpu.get_barrier_semaphore()
    for step in range(1, members):
        peer = (member + step) % members
        pl.semaphore_signal(barrier, inc=1, device_id={"expert": peer}, device_id_type=MESH)
    for step in range(1, sections):
        pl.semaphore_signal(
            barrier, inc=1, device_id={"section": (section + step) % sections}, device_id_type=MESH
        )
    pl.semaphore_wait(barrier, members + sections - 2)

    def remote(source, target, send, recv, **where):
        return pltpu.make_async_remote_copy(
            src_ref=source, dst_ref=target, send_sem=send, recv_sem=recv,
            device_id=where, device_id_type=MESH,
        )

    def dispatch(m, step):
        to = (chip + step) % CHIPS
        return remote(
            packed.at[m, to // 2], mine.at[m, chip], disp_send.at[m, step], disp_recv.at[m, chip],
            expert=to * 2 + core,
        )

    def dispatched(m, step):
        source = (chip + step) % CHIPS
        return remote(
            packed.at[m, 0], mine.at[m, source], disp_send.at[m, step], disp_recv.at[m, source],
            expert=partner,
        )

    def giving(m, step):
        to = (chip + step) % CHIPS
        return remote(
            summed.at[m, to], ret.at[m, chip], ret_send.at[m, step], ret_recv.at[m, chip],
            expert=to * 2 + core,
        )

    def given(m, step):
        source = (chip + step) % CHIPS
        return remote(
            summed.at[m, 0], ret.at[m, source], ret_send.at[m, step], ret_recv.at[m, source],
            expert=partner,
        )

    def pair(m):
        return remote(mine.at[m], other.at[m], pair_send.at[m], pair_recv.at[m], expert=partner)

    def halves(m):
        return remote(away.at[m], back.at[m], half_send.at[m], half_recv.at[m], expert=partner)

    def hop(m):
        return remote(
            leaving.at[m], states.at[m], hop_send.at[m], hop_recv.at[m],
            section=(section + 1) % sections,
        )

    head_swap = remote(head_hbm, head_other, head_send, head_recv, expert=partner)

    def cast(m, step):
        return remote(
            gathered.at[m, chip], gathered.at[m, chip], cast_send.at[m, step], cast_recv.at[m],
            section=(section + step) % sections,
        )

    def gather(m, step):
        return remote(
            gathered.at[m, chip], gathered.at[m, chip], all_send.at[m, step], all_recv.at[m, chip],
            expert=(chip + step) % CHIPS * 2 + core,
        )

    def arriving(m, step):
        source = (chip + step) % CHIPS
        return remote(
            gathered.at[m, source], gathered.at[m, source], all_send.at[m, step], all_recv.at[m, source],
            expert=partner,
        )

    def stat_to(m, step):
        to = (chip + step) % CHIPS
        return remote(
            stat_out.at[m, to], stat_in.at[m, chip], stat_send.at[m, step], stat_recv.at[m, chip],
            expert=to * 2 + core,
        )

    def stat_from(m, step):
        source = (chip + step) % CHIPS
        return remote(
            stat_out.at[m, source], stat_in.at[m, source], stat_send.at[m, step], stat_recv.at[m, source],
            expert=partner,
        )

    def plane_to(m, step):
        return remote(
            plane_out.at[m], plane_in.at[m, section], plane_send.at[m, step], plane_recv.at[m, section],
            section=(section + step) % sections,
        )

    def plane_from(m, step):
        source = (section + step) % sections
        return remote(
            plane_out.at[m], plane_in.at[m, source], plane_send.at[m, step], plane_recv.at[m, source],
            section=source,
        )

    def seq_to(step):
        return remote(
            seq_out, seq_in.at[member], seq_send.at[step], seq_recv.at[member],
            expert=(member + step) % members,
        )

    def seq_from(step):
        source = (member + step) % members
        return remote(seq_out, seq_in.at[source], seq_send.at[step], seq_recv.at[source], expert=source)

    @pl.when(section > 0)
    def _():
        head_swap.start()

    before = (iota((tok_count, tok_count), 0) < iota((tok_count, tok_count), 1)).astype(BF16)

    for m in range(micro_count):
        route = routes[m]
        first, second = route[0:1, :], route[1:2, :]

        def slots(count, shift):
            place = iota((count, tok_count), 0)
            expert = lax.shift_right_logical(place, shift)
            hit = ((expert == first) | (expert == second)).astype(F32)
            rank = jnp.dot(hit.astype(BF16), before, preferred_element_type=F32)
            return expert, jnp.where(rank == (place & 1).astype(F32), hit, 0.0)

        _, table = slots(16, 1)
        expert32, held32 = slots(32, 2)

        @pl.when(section == 0)
        def _():
            states[m] = hidden[m]

        @pl.when(section > 0)
        def _():
            hop(m).wait_recv()

        normed = rms_scale(states[m], gain[...]).astype(BF16)
        chosen = jnp.dot(table.astype(BF16), normed, preferred_element_type=F32).astype(BF16)
        packed[m] = chosen.reshape(8, 2, width)
        for step in range(1, CHIPS):
            dispatch(m, step).start()
        mine[m, chip] = packed[m, chip // 2]

        logits = lax.dot_general(router[...], normed, (((1,), (1,)), ((), ())), preferred_element_type=F32)
        row8 = iota((8, tok_count), 0)
        affinity = [
            jax.nn.sigmoid(jnp.sum(jnp.where(row8 == pick, logits, 0.0), 0, keepdims=True))
            for pick in (first, second)
        ]
        total = affinity[0] + affinity[1]
        weight = held32 * jnp.where(
            expert32 == first, affinity[0] / total, jnp.where(expert32 == second, affinity[1] / total, 0.0)
        )

        for step in range(1, CHIPS):
            dispatched(m, step).wait_recv()
        pair(m).start()
        rows[0:32] = mine[m].reshape(32, width)
        if m == 0:
            for load in loads[:3]:
                load.wait()
        pair(m).wait_recv()
        rows[32:64] = other[m].reshape(32, width)

        @pl.loop(0, 2)
        def _(j):
            span = pl.ds(pl.multiple_of(j * 256, 256), 256)
            gate_val = jnp.dot(rows[...], gate[:, span], preferred_element_type=F32)
            up_val = jnp.dot(rows[...], up[:, span], preferred_element_type=F32)
            inner[:, span] = (jax.nn.silu(gate_val) * up_val).astype(BF16)

        @pl.loop(0, 7)
        def _(j):
            span = pl.ds(pl.multiple_of(j * 512, 512), 512)
            result = jnp.dot(inner[...], down[:, span], preferred_element_type=F32)
            part[:, span] = result[0:32]
            away[m, :, :, span] = result[32:64].astype(BF16).reshape(CHIPS, 2, 512)

        halves(m).start()
        halves(m).wait_recv()
        summed[m] = (part[...] + back[m].reshape(32, width).astype(F32)).astype(BF16).reshape(CHIPS, 2, width)
        for step in range(1, CHIPS):
            giving(m, step).start()
        if m == 1:

            @pl.when(section == last)
            def _():
                for step in range(1, CHIPS):
                    gather(0, step).start()

        ret[m, chip] = summed[m, chip]

        high = weight.astype(BF16)
        middle = (weight - high.astype(F32)).astype(BF16)
        low = (weight - high.astype(F32) - middle.astype(F32)).astype(BF16)
        for step in range(1, CHIPS):
            given(m, step).wait_recv()
        returned = ret[m].reshape(32, width)
        mixed = 0.0
        for piece in (low, middle, high):
            mixed = mixed + lax.dot_general(
                piece, returned, (((0,), (0,)), ((), ())), preferred_element_type=F32
            )
        result = (states[m].astype(F32) + 2.5 * mixed).astype(BF16)
        leaving[m] = result

        @pl.when(section < last)
        def _():
            hop(m).start()

        @pl.when(section == last)
        def _():
            gathered[m, chip] = rms_scale(result, last_gain[...]).astype(BF16)
            for step in (4, 3, 5, 2, 6, 1, 7):
                cast(m, step).start()
            if m == 1:
                for step in range(1, CHIPS):
                    gather(m, step).start()

    @pl.when(section == 0)
    def _():
        head_swap.start()

    def pass_on(m):
        @pl.when(section < last)
        def _():
            cast(m, 1).wait_recv()
            for step in range(1, CHIPS):
                gather(m, step).start()

    lane = iota((8, 128), 1)

    def score(m):
        for step in range(1, CHIPS):
            arriving(m, step).wait_recv()
        if m == 0:
            loads[3].wait()
            head_swap.wait_recv()
        tokens = gathered[m].reshape(CHIPS * tok_count, width)
        target = wanted[m, :, core].reshape(CHIPS * tok_count, 1)
        scores, hits = [], 0.0
        for block, owner in ((head, member), (head_other, partner)):
            logit = lax.dot_general(
                tokens, block[...], (((1,), (1,)), ((), ())), preferred_element_type=F32
            )
            scores.append(logit)
            vocab = iota(logit.shape, 1) + (section * members + owner) * logit.shape[1]
            hits = hits + jnp.sum(jnp.where(vocab == target, logit, 0.0), -1, keepdims=True)
        peak = jnp.max(jnp.maximum(scores[0], scores[1]), -1, keepdims=True)
        total = jnp.sum(jnp.exp(scores[0] - peak) + jnp.exp(scores[1] - peak), -1, keepdims=True)
        spread = iota((CHIPS * tok_count, 128), 1)
        stats = jnp.where(spread == 0, peak, jnp.where(spread == 1, total, jnp.where(spread == 2, hits, 0.0)))
        stat_out[m] = stats.reshape(CHIPS, tok_count, 128)
        for step in range(1, CHIPS):
            stat_to(m, step).start()
        stat_in[m, chip] = stat_out[m, chip]

    def joined(box, m, count):
        pieces = [box[m, k] for k in range(count)]
        peak = pieces[0][:, 0:1]
        for piece in pieces[1:]:
            peak = jnp.maximum(peak, piece[:, 0:1])
        total, hits = 0.0, 0.0
        for piece in pieces:
            total = total + piece[:, 1:2] * jnp.exp(piece[:, 0:1] - peak)
            hits = hits + piece[:, 2:3]
        return peak, total, hits

    def across(m):
        for step in range(1, CHIPS):
            stat_from(m, step).wait_recv()
        peak, total, hits = joined(stat_in, m, CHIPS)
        stats = jnp.where(lane == 0, peak, jnp.where(lane == 1, total, jnp.where(lane == 2, hits, 0.0)))
        plane_out[m] = stats
        for step in range(1, 8):
            plane_to(m, step).start()
        plane_in[m, section] = stats

    pass_on(0)
    score(0)
    pass_on(1)
    across(0)
    score(1)
    across(1)

    sums, counts = 0.0, 0.0
    square = iota((tok_count, tok_count), 0) == iota((tok_count, tok_count), 1)
    for m in range(micro_count):
        for step in range(1, 8):
            plane_from(m, step).wait_recv()
        peak, total, hits = joined(plane_in, m, 8)
        logprob = hits - (peak + jnp.log(total))
        token_out[m : m + 1, :] = jnp.sum(jnp.where(square, logprob, 0.0), 0, keepdims=True)
        sums = sums + jnp.sum(
            jnp.where(lane == own_ids[m, member] + SEQS * m, logprob, 0.0), 0, keepdims=True
        )
        ids = all_ids[m : m + 1, :]
        for k in range(SEQS):
            found = jnp.sum((ids == k).astype(F32), -1, keepdims=True)
            counts = counts + jnp.where(lane[0:1] == SEQS * m + k, found, 0.0)
    seq_out[...] = jnp.broadcast_to(sums, (8, 128))
    for step in range(1, 32):
        seq_to(step).start()
    seq_in[member] = seq_out[...]
    for step in range(1, 32):
        seq_from(step).wait_recv()
    whole = seq_in[0, 0:1, :]
    for k in range(1, 32):
        whole = whole + seq_in[k, 0:1, :]
    mean = whole / jnp.where(counts > 0.0, counts, 1.0)
    mean_out[0:1, :] = mean[:, 0:SEQS]
    mean_out[1:2, :] = mean[:, SEQS : 2 * SEQS]

    head_swap.wait_send()
    for step in range(1, 32):
        seq_to(step).wait_send()
    for m in range(micro_count):
        for step in range(1, CHIPS):
            dispatch(m, step).wait_send()
            giving(m, step).wait_send()
            gather(m, step).wait_send()
            stat_to(m, step).wait_send()
        for step in range(1, 8):
            plane_to(m, step).wait_send()
        pair(m).wait_send()
        halves(m).wait_send()

        @pl.when(section < last)
        def _():
            hop(m).wait_send()

        @pl.when(section == last)
        def _():
            for step in range(1, 8):
                cast(m, step).wait_send()


def body(
    hidden_in, layer_gain, router, w_gate, w_up, w_down, final_gain, head, routing, targets, seq_ids
):
    micro_count, tok_count, width = hidden_in.shape
    sections, members = lax.axis_size("section"), lax.axis_size("expert")
    gate, up, down = w_gate[0], w_up[0], w_down[0]
    vmem, hbm = pl.BlockSpec(memory_space=pltpu.VMEM), pl.BlockSpec(memory_space=pl.ANY)
    block = (micro_count, CHIPS, 2, width)
    dma = pltpu.SemaphoreType.DMA
    own = (micro_count,)
    each = (micro_count, CHIPS)
    return pl.pallas_call(
        layers_kernel,
        out_shape=(
            jax.ShapeDtypeStruct((micro_count, tok_count), F32),
            jax.ShapeDtypeStruct((micro_count, SEQS), F32),
        ),
        in_specs=[vmem] * 8 + [hbm] * 4,
        out_specs=(vmem, vmem),
        scratch_shapes=[
            pltpu.VMEM(gate.shape, BF16),
            pltpu.VMEM(up.shape, BF16),
            pltpu.VMEM(down.shape, BF16),
            pltpu.VMEM(head.shape, BF16),
            pltpu.VMEM(head.shape, BF16),
            pltpu.VMEM((micro_count, CHIPS, tok_count, width), BF16),
            pltpu.VMEM((micro_count, CHIPS, tok_count, 128), F32),
            pltpu.VMEM((micro_count, CHIPS, tok_count, 128), F32),
            pltpu.VMEM((micro_count, tok_count, 128), F32),
            pltpu.VMEM((micro_count, sections, tok_count, 128), F32),
            pltpu.VMEM((8, 128), F32),
            pltpu.VMEM((members, 8, 128), F32),
            pltpu.VMEM(hidden_in.shape, BF16),
            pltpu.VMEM((micro_count, 8, 2, width), BF16),
            pltpu.VMEM(block, BF16),
            pltpu.VMEM(block, BF16),
            pltpu.VMEM((64, width), BF16),
            pltpu.VMEM((64, gate.shape[1]), BF16),
            pltpu.VMEM((32, width), F32),
            pltpu.VMEM(block, BF16),
            pltpu.VMEM(block, BF16),
            pltpu.VMEM(block, BF16),
            pltpu.VMEM(block, BF16),
            pltpu.VMEM(hidden_in.shape, BF16),
            dma((4,)),
            dma(each), dma(each),
            dma(own), dma(own),
            dma(own), dma(own),
            dma(each), dma(each),
            dma(own), dma(own),
            dma, dma,
            dma((micro_count, sections)), dma(own),
            dma(each), dma(each),
            dma(each), dma(each),
            dma((micro_count, sections)), dma((micro_count, sections)),
            dma((members,)), dma((members,)),
        ],
        compiler_params=pltpu.CompilerParams(
            collective_id=0, has_side_effects=True, vmem_limit_bytes=56 << 20
        ),
    )(
        hidden_in, layer_gain, router[0].T, routing[0].transpose(0, 2, 1), final_gain[None],
        targets.reshape(micro_count, CHIPS, 2, tok_count, 1),
        seq_ids.reshape(micro_count, members, tok_count, 1), seq_ids, gate, up, down, head,
    )


def solution(mesh):
    placed = (
        P(None, "expert", None),
        P("section", None),
        P("section", None, None),
        P("section", None, "expert"),
        P("section", None, "expert"),
        P("section", "expert", None),
        P(),
        P(("section", "expert"), None),
        P("section", None, "expert", None),
        P(),
        P(),
    )
    return jax.shard_map(
        body, mesh=mesh, in_specs=placed, out_specs=(P(None, "expert"), P()), check_vma=False
    )
```
